32 devices in a mesh: farcp: 2 (over x), nearcp: 4 (over y, core), model: 4 (over z).
Axes of the slice: x: 2, y: 2, z: 4, core: 2. Of those that a mesh axis runs over, the one named last changes fastest.
Arguments:
- raw_keys: bfloat16 [8, 8192, 8, 128], P(None, ('farcp', 'nearcp'), 'model'), may hold values from -6 to 6
- raw_values: bfloat16 [8, 8192, 8, 128], P(None, ('farcp', 'nearcp'), 'model'), may hold values from -6 to 6
- turn_angle: float32 [8192, 64], replicated, may hold values from -3.140625 to 3.140625
- key_gain: float32 [128], replicated, may hold values from 0.25 to 1.75
Outputs:
- stored_keys: bfloat16 [8, 8192, 8, 128], P(('farcp', 'nearcp'), None, 'model')
- stored_values: bfloat16 [8, 8192, 8, 128], P(('farcp', 'nearcp'), None, 'model')
- key_scale: float32 [8, 8, 128], P(('farcp', 'nearcp'), 'model')
The draws below stay inside these ranges and needn't reach their ends.
All inputs are finite; a program needn't handle non-finite values. Where the reference program divides by a largest or mean magnitude, that divisor is 1e-20 or more.
Results may differ from the reference program's by a relative error of at most 0.001.
Values may be sent and summed in bfloat16 or wider, within the bound.
A program may use at most 192 MiB of HBM per device.

```python
import jax
import jax.numpy as jnp
from jax import lax

BATCH = 8
LENGTH = 8192
KV_HEADS = 8
HEAD_SIZE = 128
HALF_HEAD = 64


def steps_of(rng, extent, cuts, low, largest):
    loudness = 1.0
    for dim, shards_of in cuts:
        draws = jax.random.uniform(jax.random.fold_in(jax.random.fold_in(rng, 6), dim), (shards_of,), jnp.float32, low / len(cuts), largest / len(cuts))
        loudness = loudness * jnp.repeat(jnp.exp(draws), extent[dim] // shards_of).reshape((-1,) + (1,) * (len(extent) - 1 - dim))
    return loudness


def gaussian(stream_key, extent, scale, reach, pieces=(), dtype=jnp.bfloat16):
    array = scale * jax.random.normal(stream_key, extent, jnp.float32)
    if pieces:
        array = array * steps_of(stream_key, extent, pieces, -0.22, 0.18)
    return jnp.clip(array, -reach, reach).astype(dtype)


def setup_inputs(seed: int = 0) -> dict:
    keys = jax.random.split(jax.random.key(seed), 5)
    return {
        "raw_keys": gaussian(keys[0], (BATCH, LENGTH, KV_HEADS, HEAD_SIZE), 1.0, 6.0, ((1, 8), (2, 4))),
        "raw_values": gaussian(keys[1], (BATCH, LENGTH, KV_HEADS, HEAD_SIZE), 1.0, 6.0, ((1, 8), (2, 4))),
        "turn_angle": jnp.clip(jax.random.uniform(keys[2], (LENGTH, HALF_HEAD), jnp.float32, -3.140625, 3.140625), -3.140625, 3.140625),
        "key_gain": jnp.clip(1.0 + 0.15 * jax.random.normal(keys[3], (HEAD_SIZE,), jnp.float32), 0.25, 1.75),
    }


def apply_rotary(vectors, angle):
    half = vectors.shape[-1] // 2
    cosine, sine = (jnp.cos(angle)[None, :, None, :], jnp.sin(angle)[None, :, None, :])
    first, second = (vectors[..., :half], vectors[..., half:])
    return jnp.concatenate([first * cosine - second * sine, second * cosine + first * sine], axis=-1)

def scale_rows(vectors, row_gain):
    return vectors * lax.rsqrt(lax.optimization_barrier(jnp.mean(vectors * vectors, axis=-1, keepdims=True)) + 1e-06) * row_gain

def prepare_keys(plain_keys, angle, key_gain):
    wide_keys = plain_keys.astype(jnp.float32)
    wide_keys = scale_rows(wide_keys, key_gain)
    return apply_rotary(wide_keys, angle)

def reference(raw_keys, raw_values, turn_angle, key_gain):
    turned_keys = prepare_keys(raw_keys, turn_angle, key_gain)
    key_scale = lax.optimization_barrier(jnp.max(jnp.abs(turned_keys), axis=1))
    narrow_keys = (turned_keys / key_scale[:, None]).astype(jnp.bfloat16)
    stored_keys = narrow_keys
    stored_values = raw_values
    return (stored_keys, stored_values, key_scale)
```

```python
import functools

import jax
import jax.numpy as jnp
from jax import lax
from jax.experimental import pallas as pl
from jax.experimental.pallas import tpu as pltpu
from jax.sharding import PartitionSpec as P

FAR, NEAR = "farcp", "nearcp"
MESH_ID = pl.DeviceIdType.MESH
TILE = 256
LANES = 128


def moved_index(index, step, size, sign):
    if size & (size - 1):
        return (index + sign * step + size) % size
    bit = 1
    while bit < size:
        if step & bit:
            index = index + bit - 2 * bit * ((index // bit) % 2)
        bit *= 2
    return index


def partner_steps(far_size, near_size):
    steps = [(f, n) for f in range(far_size) for n in range(near_size) if (f, n) != (0, 0)]
    return sorted(steps, key=lambda s: (-((s[0] > 0) + (s[1] > 1)), s))


def exchange_kernel(
    far_size, near_size, heads, keys_ref, values_ref, angle_ref, gain_ref,
    out_keys, out_values, out_scale,
    landed, cos_table, sin_table, turned, send_sem, recv_sem, local_sem,
):
    far, near = lax.axis_index(FAR), lax.axis_index(NEAR)
    me = far * near_size + near
    rows = keys_ref.shape[1]
    total_rows = landed.shape[0]
    half = angle_ref.shape[0]
    steps = partner_steps(far_size, near_size)

    def device(step, sign):
        return (
            moved_index(far, step[0], far_size, sign),
            moved_index(near, step[1], near_size, sign),
        )

    barrier = pltpu.get_barrier_semaphore()
    for step in steps:
        f, n = device(step, 1)
        pl.semaphore_signal(barrier, inc=1, device_id={FAR: f, NEAR: n}, device_id_type=MESH_ID)
    own = [
        pltpu.make_async_copy(src.at[me], dst.at[pl.ds(me * rows, rows)], local_sem.at[i])
        for i, (src, dst) in enumerate(((keys_ref, landed), (values_ref, out_values)))
    ]
    for copy in own:
        copy.start()
    pl.semaphore_wait(barrier, len(steps))

    copies = [[], []]
    for which, (src, dst) in enumerate(((keys_ref, landed), (values_ref, out_values))):
        for i, step in enumerate(steps):
            f, n = device(step, 1)
            copy = pltpu.make_async_remote_copy(
                src_ref=src.at[f * near_size + n],
                dst_ref=dst.at[pl.ds(me * rows, rows)],
                send_sem=send_sem.at[which, i],
                recv_sem=recv_sem.at[which, i],
                device_id={FAR: f, NEAR: n},
                device_id_type=MESH_ID,
            )
            copy.start()
            copies[which].append(copy)

    gain = gain_ref[...]
    other_gain = pltpu.roll(gain, half, 1)

    def fill(block, carry):
        angle = angle_ref[:, pl.ds(pl.multiple_of(block * LANES, LANES), LANES)]
        cosine, sine = jnp.cos(angle), jnp.sin(angle)
        cosine = jnp.concatenate([cosine, cosine], axis=0).T * gain
        sine = jnp.concatenate([-sine, sine], axis=0).T * other_gain
        for head in range(heads):
            place = pl.ds(block * (LANES * heads) + head, LANES, stride=heads)
            cos_table[place, :] = cosine
            sin_table[place, :] = sine
        return carry

    lax.fori_loop(0, total_rows // (heads * LANES), fill, 0)

    def prepare(owner, largest):
        def body(i, largest):
            place = pl.ds(pl.multiple_of(owner * rows + i * TILE, TILE), TILE)
            x = landed[place, :].astype(jnp.float32)
            mean = jnp.sum(x * x, axis=-1, keepdims=True) * (1.0 / x.shape[-1])
            x = x * lax.rsqrt(mean + 1e-06)
            t = x * cos_table[place, :] + pltpu.roll(x, half, 1) * sin_table[place, :]
            turned[place, :] = t
            return jnp.maximum(largest, jnp.max(jnp.abs(t).reshape(TILE // 8, 8, LANES), axis=0))

        return lax.fori_loop(0, rows // TILE, body, largest)

    largest = jnp.zeros((8, LANES), jnp.float32)
    own[0].wait()
    largest = prepare(me, largest)
    for i in reversed(range(len(steps))):
        copies[0][i].wait_recv()
        f, n = device(steps[i], -1)
        largest = prepare(f * near_size + n, largest)

    head_of = lax.broadcasted_iota(jnp.int32, (8, LANES), 0) % heads
    scale = jnp.zeros((8, LANES), jnp.float32)
    for head in range(heads):
        top = jnp.max(jnp.where(head_of == head, largest, 0.0), axis=0, keepdims=True)
        out_scale[pl.ds(head, 1), :] = top
        scale = jnp.where(head_of == head, top, scale)
    inverse = (1.0 / scale)[None]

    def narrow(i, carry):
        place = pl.ds(pl.multiple_of(i * TILE, TILE), TILE)
        t = turned[place, :].reshape(TILE // 8, 8, LANES) * inverse
        out_keys[place, :] = t.reshape(TILE, LANES).astype(out_keys.dtype)
        return carry

    lax.fori_loop(0, total_rows // TILE, narrow, 0)

    own[1].wait()
    for copy in copies[1]:
        copy.wait_recv()
    for group in copies:
        for copy in group:
            copy.wait_send()


def place_kernel(keys_ref, values_ref, out_keys, out_values, sem):
    copies = [
        pltpu.make_async_copy(keys_ref, out_keys, sem.at[0]),
        pltpu.make_async_copy(values_ref, out_values, sem.at[1]),
    ]
    for copy in copies:
        copy.start()
    for copy in copies:
        copy.wait()


def local(far_size, near_size, raw_keys, raw_values, turn_angle, key_gain):
    sequences, positions, heads, size = raw_keys.shape
    devices = far_size * near_size
    rows = positions * heads
    total = rows * devices
    steps = devices - 1
    flat = (sequences, rows, size)
    whole = pltpu.VMEM((total, size), raw_keys.dtype)
    keys, values, scale = pl.pallas_call(
        functools.partial(exchange_kernel, far_size, near_size, heads),
        out_shape=(whole, whole, jax.ShapeDtypeStruct((heads, size), jnp.float32)),
        in_specs=[
            pl.BlockSpec(memory_space=pl.ANY),
            pl.BlockSpec(memory_space=pl.ANY),
            pl.BlockSpec(memory_space=pltpu.VMEM),
            pl.BlockSpec(memory_space=pltpu.VMEM),
        ],
        out_specs=(
            pl.BlockSpec(memory_space=pltpu.VMEM),
            pl.BlockSpec(memory_space=pltpu.VMEM),
            pl.BlockSpec(memory_space=pltpu.VMEM),
        ),
        scratch_shapes=[
            pltpu.VMEM((total, size), raw_keys.dtype),
            pltpu.VMEM((total, size), jnp.float32),
            pltpu.VMEM((total, size), jnp.float32),
            pltpu.VMEM((total, size), jnp.float32),
            pltpu.SemaphoreType.DMA((2, steps)),
            pltpu.SemaphoreType.DMA((2, steps)),
            pltpu.SemaphoreType.DMA((2,)),
        ],
        compiler_params=pltpu.CompilerParams(
            collective_id=0, has_side_effects=True, vmem_limit_bytes=48 * 1024 * 1024
        ),
        name="exchange",
    )(raw_keys.reshape(flat), raw_values.reshape(flat), turn_angle.T, key_gain.reshape(1, size))
    out = jax.ShapeDtypeStruct((total, size), raw_keys.dtype)
    keys, values = pl.pallas_call(
        place_kernel,
        out_shape=(out, out),
        in_specs=[pl.BlockSpec(memory_space=pltpu.VMEM)] * 2,
        out_specs=[pl.BlockSpec(memory_space=pl.ANY)] * 2,
        scratch_shapes=[pltpu.SemaphoreType.DMA((2,))],
        compiler_params=pltpu.CompilerParams(vmem_limit_bytes=12 * 1024 * 1024),
        name="place",
    )(keys, values)
    full = (1, positions * devices, heads, size)
    return keys.reshape(full), values.reshape(full), scale.reshape(1, heads, size)


def solution(mesh):
    in_specs = (
        P(None, (FAR, NEAR), "model", None),
        P(None, (FAR, NEAR), "model", None),
        P(),
        P(),
    )
    out_specs = (
        P((FAR, NEAR), None, "model", None),
        P((FAR, NEAR), None, "model", None),
        P((FAR, NEAR), "model", None),
    )
    body = functools.partial(local, mesh.shape[FAR], mesh.shape[NEAR])
    return jax.shard_map(body, mesh=mesh, in_specs=in_specs, out_specs=out_specs, check_vma=False)
```

```python
import functools

import jax
import jax.numpy as jnp
from jax import lax
from jax.experimental import pallas as pl
from jax.experimental.pallas import tpu as pltpu
from jax.sharding import PartitionSpec as P

FAR, NEAR = "farcp", "nearcp"
MESH_ID = pl.DeviceIdType.MESH
TILE = 256
PARTS = 1
WRITES = 4
LANES = 128


def moved_index(index, step, size, sign):
    if size & (size - 1):
        return (index + sign * step + size) % size
    bit = 1
    while bit < size:
        index = index + ((step // bit) % 2) * (bit - 2 * bit * ((index // bit) % 2))
        bit *= 2
    return index


def partner_orders(far_size, near_size):
    both, first, second, same = [], [], [], []
    for step in range(1, far_size * near_size):
        far, chip = step // near_size > 0, step % near_size > 1
        (both if far and chip else first if far else second if chip else same).append(step)
    orders = []
    for lists in ((both, first, second), (first, both, second)):
        order = []
        for turn in range(max(map(len, lists))):
            order += [steps[turn] for steps in lists if turn < len(steps)]
        orders.append(order + same)
    return orders


def exchange_kernel(
    far_size, near_size, heads, keys_ref, values_ref, turn_ref, gain_ref,
    out_keys, out_values, out_scale,
    angle_ref, landed, cos_table, sin_table, turned, send_sem, recv_sem, local_sem,
):
    far, near = lax.axis_index(FAR), lax.axis_index(NEAR)
    me = far * near_size + near
    rows = keys_ref.shape[1]
    total_rows = landed.shape[0]
    half = angle_ref.shape[0]
    even, odd = partner_orders(far_size, near_size)
    part = rows // PARTS

    def device(step, sign):
        return (
            moved_index(far, step // near_size, far_size, sign),
            moved_index(near, step % near_size, near_size, sign),
        )

    barrier = pltpu.get_barrier_semaphore()
    for step in even:
        f, n = device(step, 1)
        pl.semaphore_signal(barrier, inc=1, device_id={FAR: f, NEAR: n}, device_id_type=MESH_ID)
    angles = pltpu.make_async_copy(turn_ref, angle_ref, local_sem.at[2])
    angles.start()
    own = [
        pltpu.make_async_copy(src.at[me], dst.at[pl.ds(me * rows, rows)], local_sem.at[i])
        for i, (src, dst) in enumerate(((keys_ref, landed), (values_ref, out_values)))
    ]
    for copy in own:
        copy.start()

    def remote(which, piece, step):
        src, dst = ((keys_ref, landed), (values_ref, out_values))[which]
        f, n = device(step, 1)
        return pltpu.make_async_remote_copy(
            src_ref=src.at[f * near_size + n, pl.ds(piece * part, part)],
            dst_ref=dst.at[pl.ds(me * rows + piece * part, part)],
            send_sem=send_sem.at[which, piece, step],
            recv_sem=recv_sem.at[which, piece, step],
            device_id={FAR: f, NEAR: n},
            device_id_type=MESH_ID,
        )

    pl.semaphore_wait(barrier, len(even))
    for which in range(2):
        for piece in range(PARTS):
            for a, b in zip(even, odd):
                remote(which, piece, a + (b - a) * (me % 2)).start()

    angles.wait()
    gain = gain_ref[...]
    other_gain = pltpu.roll(gain, half, 1)

    def fill(block, carry):
        angle = angle_ref[:, pl.ds(pl.multiple_of(block * LANES, LANES), LANES)]
        cosine, sine = jnp.cos(angle), jnp.sin(angle)
        cosine = jnp.concatenate([cosine, cosine], axis=0).T * gain
        sine = jnp.concatenate([-sine, sine], axis=0).T * other_gain
        for head in range(heads):
            place = pl.ds(block * (LANES * heads) + head, LANES, stride=heads)
            cos_table[place, :] = cosine
            sin_table[place, :] = sine
        return carry

    lax.fori_loop(0, total_rows // (heads * LANES), fill, 0)

    def prepare(owner, largest):
        def body(i, largest):
            place = pl.ds(pl.multiple_of(owner * rows + i * TILE, TILE), TILE)
            x = landed[place, :].astype(jnp.float32)
            mean = jnp.sum(x * x, axis=-1, keepdims=True) * (1.0 / x.shape[-1])
            x = x * lax.rsqrt(mean + 1e-06)
            t = x * cos_table[place, :] + pltpu.roll(x, half, 1) * sin_table[place, :]
            turned[place, :] = t
            return jnp.maximum(largest, jnp.max(jnp.abs(t).reshape(TILE // 8, 8, LANES), axis=0))

        return lax.fori_loop(0, rows // TILE, body, largest)

    largest = jnp.zeros((8, LANES), jnp.float32)
    own[0].wait()
    largest = prepare(me, largest)
    for step in even[::-1]:
        for piece in range(PARTS):
            remote(0, piece, step).wait_recv()
        f, n = device(step, -1)
        largest = prepare(f * near_size + n, largest)

    head_of = lax.broadcasted_iota(jnp.int32, (8, LANES), 0) % heads
    scale = jnp.zeros((8, LANES), jnp.float32)
    for head in range(heads):
        top = jnp.max(jnp.where(head_of == head, largest, 0.0), axis=0, keepdims=True)
        out_scale[pl.ds(head, 1), :] = top
        scale = jnp.where(head_of == head, top, scale)
    inverse = (1.0 / scale)[None]

    def narrow(i, carry):
        place = pl.ds(pl.multiple_of(i * TILE, TILE), TILE)
        t = turned[place, :].reshape(TILE // 8, 8, LANES) * inverse
        out_keys[place, :] = t.reshape(TILE, LANES).astype(out_keys.dtype)
        return carry

    lax.fori_loop(0, total_rows // TILE, narrow, 0)

    own[1].wait()
    for piece in range(PARTS):
        for step in even:
            remote(1, piece, step).wait_recv()
    for which in range(2):
        for piece in range(PARTS):
            for step in even:
                remote(which, piece, step).wait_send()


def place_kernel(keys_ref, values_ref, scale_ref, out_keys, out_values, out_scale, sem):
    part = keys_ref.shape[0] // WRITES
    copies = [pltpu.make_async_copy(scale_ref, out_scale, sem.at[2, 0])]
    for i, (src, dst) in enumerate(((keys_ref, out_keys), (values_ref, out_values))):
        for j in range(WRITES):
            place = pl.ds(j * part, part)
            copies.append(pltpu.make_async_copy(src.at[place], dst.at[place], sem.at[i, j]))
    for copy in copies:
        copy.start()
    for copy in copies:
        copy.wait()


def local(far_size, near_size, raw_keys, raw_values, turn_angle, key_gain):
    sequences, positions, heads, size = raw_keys.shape
    devices = far_size * near_size
    rows = positions * heads
    total = rows * devices
    flat = (sequences, rows, size)
    whole = pltpu.VMEM((total, size), raw_keys.dtype)
    keys, values, scale = pl.pallas_call(
        functools.partial(exchange_kernel, far_size, near_size, heads),
        out_shape=(whole, whole, pltpu.VMEM((heads, size), jnp.float32)),
        in_specs=[
            pl.BlockSpec(memory_space=pl.ANY),
            pl.BlockSpec(memory_space=pl.ANY),
            pl.BlockSpec(memory_space=pl.ANY),
            pl.BlockSpec(memory_space=pltpu.VMEM),
        ],
        out_specs=(
            pl.BlockSpec(memory_space=pltpu.VMEM),
            pl.BlockSpec(memory_space=pltpu.VMEM),
            pl.BlockSpec(memory_space=pltpu.VMEM),
        ),
        scratch_shapes=[
            pltpu.VMEM((size // 2, total // heads), jnp.float32),
            pltpu.VMEM((total, size), raw_keys.dtype),
            pltpu.VMEM((total, size), jnp.float32),
            pltpu.VMEM((total, size), jnp.float32),
            pltpu.VMEM((total, size), jnp.float32),
            pltpu.SemaphoreType.DMA((2, PARTS, devices)),
            pltpu.SemaphoreType.DMA((2, PARTS, devices)),
            pltpu.SemaphoreType.DMA((3,)),
        ],
        compiler_params=pltpu.CompilerParams(
            collective_id=0, has_side_effects=True, vmem_limit_bytes=48 * 1024 * 1024
        ),
        name="exchange",
    )(raw_keys.reshape(flat), raw_values.reshape(flat), turn_angle.T, key_gain.reshape(1, size))
    out = jax.ShapeDtypeStruct((total, size), raw_keys.dtype)
    keys, values, scale = pl.pallas_call(
        place_kernel,
        out_shape=(out, out, jax.ShapeDtypeStruct((heads, size), jnp.float32)),
        in_specs=[pl.BlockSpec(memory_space=pltpu.VMEM)] * 3,
        out_specs=[pl.BlockSpec(memory_space=pl.ANY)] * 3,
        scratch_shapes=[pltpu.SemaphoreType.DMA((3, WRITES))],
        compiler_params=pltpu.CompilerParams(vmem_limit_bytes=12 * 1024 * 1024),
        name="place",
    )(keys, values, scale)
    full = (1, positions * devices, heads, size)
    return keys.reshape(full), values.reshape(full), scale.reshape(1, heads, size)


def solution(mesh):
    in_specs = (
        P(None, (FAR, NEAR), "model", None),
        P(None, (FAR, NEAR), "model", None),
        P(),
        P(),
    )
    out_specs = (
        P((FAR, NEAR), None, "model", None),
        P((FAR, NEAR), None, "model", None),
        P((FAR, NEAR), "model", None),
    )
    body = functools.partial(local, mesh.shape[FAR], mesh.shape[NEAR])
    return jax.shard_map(body, mesh=mesh, in_specs=in_specs, out_specs=out_specs, check_vma=False)
```
